512 devices in a mesh: dom: 128 (over z, y, core), level: 4 (over x).
Axes of the slice: x: 4, y: 4, z: 16, core: 2. Of those that a mesh axis runs over, the one named last changes fastest.
Arguments:
- dg_values: bfloat16 [1572864, 384], P(('dom', 'level')), may hold values from -6 to 6
- stiff_mu: bfloat16 [384, 384], replicated, may hold values from -0.1 to 2, as said below
- stiff_lam: bfloat16 [384, 384], replicated, may hold values from -0.1 to 2, as said below
- coef_mu: float32 [1572864], P(('dom', 'level')), may hold values from 0.25 to 4
- coef_lam: float32 [1572864], P(('dom', 'level')), may hold values from 0.25 to 4
- elem_count: int32 [512], P(('dom', 'level')), may hold values from 384 to 3072, as said below
- elem_block: int32 [3, 1572864], P(None, ('dom', 'level')), may hold values from 0 to 1023
- share_map: int32 [512, 8, 32], P(('dom', 'level')), may hold values from 0 to 1024, as said below
- hang_child: int32 [512, 64], P(('dom', 'level')), may hold values from 0 to 1024, as said below
- hang_parent: int32 [512, 64, 2], P(('dom', 'level')), may hold values from 0 to 1023
Outputs:
- projected: float32 [3, 524288, 128], P(None, ('dom', 'level'))
- energy: float32 [], replicated
The draws below stay inside these ranges and needn't reach their ends.
Inputs may be any that keep to these rules, and one draw needn't show every extreme that they name: `elem_count`: between 384 and 3072; one device, drawn anew, holds exactly 3072. `share_map`: entry [d, o, s] is the local block that device d shares with rank r + off_o of its level through slot s (offsets as in the reference program); 1024 marks an empty slot. Slots agree in pairs: [d, o, s] is live exactly when the partner's [d2, o', s] is live, and they name the same DoF block. Slots toward ranks outside 0 to 127 are empty. For every offset some rank pair fills all 32 slots. `hang_child`: on each device of level index 1 or more, 64 distinct blocks below 1024; on devices of level index 0 every entry is 1024 (no hanging blocks). `hang_parent`: block numbers on the device of the same rank and the next lower level index; unused on level index 0. `stiff_mu`: Symmetric. `stiff_lam`: Symmetric.
All inputs are finite; a program needn't handle non-finite values.
Results may differ from the reference program's by a relative error of at most 0.0003.
Values sent between devices are 32-bit elements; how exact they have to be, the bound alone decides.
A program may use at most 64 MiB of HBM per device.

```python
import math
import jax
import jax.numpy as jnp
from jax import lax

BLK = 128
EDOF = 384
E_CAP = 3072
NBC = 1024
W = 4
SLOT = 32
H = 64
RANKS = 128
LEVELS = 4
ELEMS = 1572864


def stiffness_draw(key, salt):
    first_key, second_key = jax.random.split(jax.random.fold_in(key, salt))
    noise = jax.random.truncated_normal(first_key, -4.0, 4.0, (EDOF, EDOF), jnp.float32)
    noise = (noise + noise.T) * (0.3 / (2.0 * EDOF) ** 0.5)
    diagonal = jax.random.uniform(second_key, (EDOF,), jnp.float32, 0.8, 1.6)
    return (noise + jnp.diag(diagonal)).astype(jnp.bfloat16)


def draw_stiff_mu(key, part):
    return stiffness_draw(key, 101)


def draw_stiff_lam(key, part):
    return stiffness_draw(key, 202)


def draw_elem_count(key, part):
    first_key, second_key = jax.random.split(jax.random.fold_in(key, 11))
    raw = jax.random.randint(first_key, (RANKS * LEVELS,), 0, 1024)
    spread = raw * raw // 1024
    counts = E_CAP // 8 + spread * (E_CAP - E_CAP // 8) // 1023
    chosen = jax.random.randint(second_key, (), 0, RANKS * LEVELS)
    return jnp.where(jnp.arange(RANKS * LEVELS) == chosen, E_CAP, counts).astype(jnp.int32)


def draw_share_map(key, part):
    first_key, second_key, third_key = jax.random.split(jax.random.fold_in(key, 23), 3)
    counts = jax.random.randint(first_key, (RANKS, LEVELS, W), 1, SLOT + 1)
    chosen = jax.random.randint(second_key, (LEVELS, W), 0, RANKS - W)
    rank_ids = jnp.arange(RANKS, dtype=jnp.int32)
    counts = jnp.where(rank_ids[:, None, None] == chosen[None, :, :], SLOT, counts)
    offsets = jnp.concatenate([jnp.arange(1, W + 1), -jnp.arange(1, W + 1)]).astype(jnp.int32)
    partner = rank_ids[:, None] + offsets[None, :]
    inside = (partner >= 0) & (partner < RANKS)
    lower = jnp.clip(jnp.minimum(rank_ids[:, None], partner), 0, RANKS - 1)
    distance = jnp.abs(offsets) - 1
    pair_counts = counts[lower[:, None, :], jnp.arange(LEVELS)[None, :, None], distance[None, None, :]]
    slot_ids = jnp.arange(SLOT, dtype=jnp.int32)
    live_slots = (slot_ids[None, None, None, :] < pair_counts[..., None]) & inside[:, None, :, None]
    picks = jax.random.randint(third_key, (RANKS, LEVELS, 2 * W, SLOT), 0, NBC)
    result = jnp.where(live_slots, picks, NBC)
    return result.reshape(RANKS * LEVELS, 2 * W, SLOT).astype(jnp.int32)


def draw_hang_child(key, part):
    keys = jax.random.split(jax.random.fold_in(key, 37), RANKS * LEVELS)
    chosen = jax.vmap(lambda single: jax.random.permutation(single, NBC)[:H])(keys)
    level_ids = jnp.arange(RANKS * LEVELS) % LEVELS
    return jnp.where(level_ids[:, None] == 0, NBC, chosen).astype(jnp.int32)


def set_ends(array, stream_key, least, top_value):
    spot = [jax.random.randint(jax.random.fold_in(stream_key, axis), (), 0, length) for axis, length in enumerate(array.shape)]
    longest = array.shape.index(max(array.shape))
    beside = spot[:longest] + [(spot[longest] + 1) % array.shape[longest]] + spot[longest + 1:]
    return array.at[tuple(spot)].set(least).at[tuple(beside)].set(top_value)


def levels(stream_key, extent, cuts, least, largest):
    def one(position, blocks):
        draws = jax.random.uniform(jax.random.fold_in(jax.random.fold_in(stream_key, 6), position), (blocks,), jnp.float32, least / len(cuts), largest / len(cuts))
        return jnp.repeat(jnp.exp(draws), extent[position] // blocks).reshape((-1,) + (1,) * (len(extent) - position - 1))

    factor_of = one(*cuts[0])
    for cut in cuts[1:]:
        factor_of = factor_of * one(*cut)
    return factor_of


def centred(key, dims, scale, bound, cuts=(), held_as=jnp.bfloat16):
    drawn = jax.random.normal(key, dims, jnp.float32) * scale
    if len(cuts) > 0:
        drawn = levels(key, dims, cuts, -0.22, 0.18) * drawn
    return jnp.clip(drawn, min=-bound, max=bound).astype(held_as)


def setup_inputs(seed: int = 0) -> dict:
    streams_of = jax.random.split(jax.random.key(seed), 11)
    dg_values = centred(streams_of[0], (ELEMS, EDOF), 1.0, 6.0, ((0, 512),))
    stiff_mu = draw_stiff_mu(jax.random.fold_in(streams_of[10], 71), 0)
    stiff_lam = draw_stiff_lam(jax.random.fold_in(streams_of[10], 71), 0)
    coef_mu = jnp.clip(jnp.exp(math.log(4.0) - 2.7725887 * jax.random.uniform(streams_of[3], (ELEMS,), jnp.float32) ** levels(streams_of[3], (ELEMS,), ((0, 512),), -0.2, 0.2)), 0.25, 4.0)
    coef_lam = jnp.clip(jnp.exp(math.log(4.0) - 2.7725887 * jax.random.uniform(streams_of[4], (ELEMS,), jnp.float32) ** levels(streams_of[4], (ELEMS,), ((0, 512),), -0.2, 0.2)), 0.25, 4.0)
    elem_count = draw_elem_count(jax.random.fold_in(streams_of[10], 71), 0)
    elem_block = set_ends(jax.random.randint(streams_of[6], (3, ELEMS), 0, NBC), jax.random.fold_in(streams_of[6], 1), 0, NBC - 1).astype(jnp.int32)
    share_map = draw_share_map(jax.random.fold_in(streams_of[10], 71), 0)
    hang_child = draw_hang_child(jax.random.fold_in(streams_of[10], 71), 0)
    hang_parent = set_ends(jax.random.randint(streams_of[9], (RANKS * LEVELS, H, 2), 0, NBC), jax.random.fold_in(streams_of[9], 1), 0, NBC - 1).astype(jnp.int32)
    return {"dg_values": dg_values, "stiff_mu": stiff_mu, "stiff_lam": stiff_lam, "coef_mu": coef_mu, "coef_lam": coef_lam, "elem_count": elem_count, "elem_block": elem_block, "share_map": share_map, "hang_child": hang_child, "hang_parent": hang_parent}


def reference(dg_values, stiff_mu, stiff_lam, coef_mu, coef_lam, elem_count, elem_block, share_map, hang_child, hang_parent):
    shards = RANKS * LEVELS
    values_all = dg_values.reshape(shards, E_CAP, EDOF)
    shear_all = coef_mu.reshape(shards, E_CAP)
    volume_all = coef_lam.reshape(shards, E_CAP)
    block_all = elem_block.reshape(3, shards, E_CAP).transpose(1, 0, 2)

    def one_device(packed):
        values_row, shear_row, volume_row, live_count, block_ids = packed
        forces = shear_row[:, None] * jnp.dot(values_row, stiff_mu, preferred_element_type=jnp.float32)
        forces = forces + volume_row[:, None] * jnp.dot(values_row, stiff_lam, preferred_element_type=jnp.float32)
        live_rows = jnp.arange(E_CAP) < live_count
        forces = jnp.where(live_rows[:, None], forces, jnp.float32(0.0))
        energy_part = jnp.sum(values_row.astype(jnp.float32) * forces)
        sums = [jax.ops.segment_sum(forces[:, component * BLK:(component + 1) * BLK], block_ids[component], num_segments=NBC + 1) for component in range(3)]
        return jnp.stack(sums), energy_part

    local_blocks, energies = lax.map(one_device, (values_all, shear_all, volume_all, elem_count, block_all))
    energy = 0.5 * jnp.sum(energies) / jnp.float32(EDOF * ELEMS)
    local_blocks = local_blocks.reshape(RANKS, LEVELS, 3, NBC + 1, BLK)
    maps = share_map.reshape(RANKS, LEVELS, 2 * W, SLOT)
    offsets = [step + 1 for step in range(W)] + [-(step + 1) for step in range(W)]
    rank_ids = jnp.arange(RANKS, dtype=jnp.int32)
    level_ids = jnp.arange(LEVELS, dtype=jnp.int32)
    assembled = local_blocks
    for slot_index in range(2 * W):
        opposite = (slot_index + W) % (2 * W)
        partner = rank_ids + offsets[slot_index]
        inside = (partner >= 0) & (partner < RANKS)
        safe_rank = jnp.clip(partner, 0, RANKS - 1).astype(jnp.int32)
        partner_ids = maps[safe_rank][:, :, opposite, :]
        arrived = local_blocks[safe_rank[:, None, None], level_ids[None, :, None], :, partner_ids]
        arrived = jnp.where(inside[:, None, None, None, None], arrived, jnp.float32(0.0))
        targets = maps[:, :, slot_index, :]
        assembled = assembled.at[rank_ids[:, None, None], level_ids[None, :, None], :, targets].add(arrived)
    assembled = assembled.at[:, :, :, NBC, :].set(jnp.float32(0.0))
    coarse = jnp.concatenate([jnp.zeros_like(assembled[:, :1]), assembled[:, :-1]], axis=1)
    parents = hang_parent.reshape(RANKS, LEVELS, H, 2)
    first_parent = coarse[rank_ids[:, None, None], level_ids[None, :, None], :, parents[..., 0]]
    second_parent = coarse[rank_ids[:, None, None], level_ids[None, :, None], :, parents[..., 1]]
    child_values = 0.5 * (first_parent + second_parent)
    children = hang_child.reshape(RANKS, LEVELS, H)
    projected = assembled.at[rank_ids[:, None, None], level_ids[None, :, None], :, children].set(child_values)
    projected = projected[:, :, :, :NBC, :].reshape(shards, 3, NBC, BLK).transpose(1, 0, 2, 3).reshape(3, shards * NBC, BLK)
    return projected, energy
```

```python
import functools

import jax
import jax.numpy as jnp
from jax import lax
from jax.experimental import pallas as pl
from jax.experimental.pallas import tpu as pltpu
from jax.sharding import PartitionSpec as P

MESH = pl.DeviceIdType.MESH
VMEM = pltpu.VMEM
F32 = jnp.float32
BF16 = jnp.bfloat16
CHUNK = 256
TILE = 256


def split(x):
    high = x.astype(BF16)
    low = (x - high.astype(F32)).astype(BF16)
    return jnp.concatenate([high, low], axis=1)


def one_hot(base, rows, ids):
    near = ids - base
    row = lax.broadcasted_iota(jnp.int32, (rows, ids.shape[1]), 0)
    return (row == near).astype(F32).astype(BF16)


def local_kernel(count, v, kmu, klam, mu, lam, ids, blocks, energy, terms):
    elements, width = v.shape
    size = width // 3
    rows = mu.shape[0]
    place = lax.broadcasted_iota(jnp.int32, (rows, 128), 0) * 128
    place = place + lax.broadcasted_iota(jnp.int32, (rows, 128), 1)
    live = place < count[0]
    mu_t = jnp.transpose(jnp.where(live, mu[...], 0.0))
    lam_t = jnp.transpose(jnp.where(live, lam[...], 0.0))
    total = jnp.zeros((8, size), F32)
    for g in range(elements // CHUNK):
        at = pl.ds(g * CHUNK, CHUNK)
        part = v[at, :]
        by_mu = jnp.dot(part, kmu[...], preferred_element_type=F32)
        by_lam = jnp.dot(part, klam[...], preferred_element_type=F32)
        n = CHUNK // 128
        a = jnp.concatenate([mu_t[:, g * n + i : g * n + i + 1] for i in range(n)], axis=0)
        b = jnp.concatenate([lam_t[:, g * n + i : g * n + i + 1] for i in range(n)], axis=0)
        forces = a * by_mu + b * by_lam
        work = part.astype(F32) * forces
        for c in range(3):
            cols = slice(c * size, (c + 1) * size)
            total = total + jnp.sum(work[:, cols].reshape(CHUNK // 8, 8, size), axis=0)
            terms[c, at, :] = split(forces[:, cols])
    energy[...] = jnp.sum(total, axis=0, keepdims=True)

    tiles = blocks.shape[1] // TILE

    def tile(i, carry):
        c = i // tiles
        base = lax.rem(i, tiles) * TILE
        hot = one_hot(base, TILE, ids[pl.ds(c, 1), :])
        both = jnp.dot(hot, terms[c], preferred_element_type=F32)
        blocks[c, pl.ds(base, TILE), :] = both[:, :size] + both[:, size:]
        return carry

    lax.fori_loop(0, 3 * tiles, tile, 0)


def exchange_kernel(
    share, blocks, slot_ids, parents, child_ids, energy_part,
    out, energy,
    summed, gather, arrived, child_out, child_in, wanted_in, wanted, mine, plane, column,
    share_send, share_recv, child_send, child_recv, wanted_sem, plane_send, plane_recv, column_send, column_recv,
):
    dom, level = lax.axis_index("dom"), lax.axis_index("level")
    ranks, levels = lax.axis_size("dom"), lax.axis_size("level")
    slots, each = share.shape
    half = slots // 2
    size = blocks.shape[2]
    count = blocks.shape[1]
    slab = ranks // 16
    offsets = [o + 1 for o in range(half)] + [-(o + 1) for o in range(half)]
    near = [(lax.rem(dom + off + ranks, ranks), level) for off in offsets]
    finer = (dom, lax.rem(level + 1, levels))
    coarser = (dom, lax.rem(level + levels - 1, levels))
    first = lax.rem(dom, slab) * levels + level
    z = dom // slab
    group = slab * levels
    in_plane = []
    for k in range(1, group):
        other = lax.rem(first + k, group)
        in_plane.append((z * slab + other // levels, lax.rem(other, levels)))
    depth = ranks // slab
    in_column = [(lax.rem(z + k, depth) * slab + lax.rem(dom, slab), level) for k in range(1, depth)]

    greeted = near + [finer, coarser] + in_plane + in_column
    barrier = pltpu.get_barrier_semaphore()
    for device in greeted:
        pl.semaphore_signal(barrier, inc=1, device_id=device, device_id_type=MESH)
    pl.semaphore_wait(barrier, len(greeted))

    def remote(src, dst, send, recv, device):
        return pltpu.make_async_remote_copy(
            src_ref=src, dst_ref=dst, send_sem=send, recv_sem=recv, device_id=device, device_id_type=MESH
        )

    ask = remote(parents, wanted_in, wanted_sem.at[0], wanted_sem.at[1], coarser)
    ask.start()
    plane_copies = [
        remote(energy_part, plane.at[k], plane_send, plane_recv, device) for k, device in enumerate(in_plane)
    ]
    for copy in plane_copies:
        copy.start()

    shares = []
    for c in range(3):
        for o in range(slots):
            def pick(s, carry):
                gather[c, o, pl.ds(s, 1), :] = blocks[c, pl.ds(jnp.minimum(share[o, s], count - 1), 1), :]
                return carry

            lax.fori_loop(0, each, pick, 0, unroll=True)
        for o in range(slots):
            there = (o + half) % slots
            copy = remote(gather.at[c, o], arrived.at[c, there], share_send.at[c, o], share_recv.at[c, there], near[o])
            copy.start()
            shares.append(copy)

    ask.wait()
    fetch = pltpu.make_async_copy(wanted_in, wanted, wanted_sem.at[2])
    fetch.start()
    remote(plane, plane, plane_send, plane_recv, finer).wait_recv()
    level_sum = energy_part[...] + jnp.sum(plane[...], axis=0)
    mine[...] = level_sum
    column_copies = [
        remote(mine, column.at[k], column_send, column_recv, device) for k, device in enumerate(in_column)
    ]
    for copy in column_copies:
        copy.start()
    fetch.wait()

    hot = one_hot(0, count, slot_ids[...])
    children = []
    for c in range(3):
        for o in range(slots):
            shares[c * slots + o].wait_recv()
        got = arrived[c].reshape(slots * each, size)
        both = jnp.dot(hot, split(got), preferred_element_type=F32)
        summed[c] = blocks[c] + (both[:, :size] + both[:, size:])

        def pair(h, carry):
            one = summed[c, pl.ds(wanted[0, h], 1), :]
            two = summed[c, pl.ds(wanted[1, h], 1), :]
            child_out[c, pl.ds(h, 1), :] = 0.5 * (one + two)
            return carry

        lax.fori_loop(0, wanted.shape[1], pair, 0, unroll=True)
        copy = remote(child_out.at[c], child_in.at[c], child_send.at[c], child_recv.at[c], finer)
        copy.start()
        children.append(copy)

    hangs = one_hot(0, count, child_ids[...])
    keep = 1.0 - jnp.sum(hangs.astype(F32), axis=1, keepdims=True)
    for c in range(3):
        children[c].wait_recv()
        both = jnp.dot(hangs, split(child_in[c]), preferred_element_type=F32)
        out[c] = keep * summed[c] + (both[:, :size] + both[:, size:])

    remote(column, column, column_send, column_recv, finer).wait_recv()
    everything = mine[...] + jnp.sum(column[...], axis=0)
    energy[...] = jnp.sum(everything, axis=1, keepdims=True)
    for copy in plane_copies + column_copies + shares + children:
        copy.wait_send()


def shards(
    dg_values, stiff_mu, stiff_lam, coef_mu, coef_lam, elem_count, elem_block, share_map, hang_child, hang_parent
):
    elements, width = dg_values.shape
    size = width // 3
    count = elements // 3
    in_vmem = pl.BlockSpec(memory_space=VMEM)
    in_smem = pl.BlockSpec(memory_space=pltpu.SMEM)
    blocks, energy_part = pl.pallas_call(
        local_kernel,
        out_shape=[jax.ShapeDtypeStruct((3, count, size), F32), jax.ShapeDtypeStruct((1, size), F32)],
        in_specs=[in_smem] + [in_vmem] * 6,
        out_specs=[in_vmem, in_vmem],
        scratch_shapes=[VMEM((3, elements, 2 * size), BF16)],
    )(
        elem_count, dg_values, stiff_mu, stiff_lam,
        coef_mu.reshape(-1, 128), coef_lam.reshape(-1, 128), elem_block,
    )
    slots, each = share_map.shape[1:]
    hangs = hang_child.shape[1]
    ranks, levels = lax.axis_size("dom"), lax.axis_size("level")
    group, depth = ranks // 16 * levels, 16
    sem = pltpu.SemaphoreType.DMA
    projected, energy = pl.pallas_call(
        exchange_kernel,
        out_shape=[jax.ShapeDtypeStruct((3, count, size), F32), jax.ShapeDtypeStruct((1, 1), F32)],
        in_specs=[in_smem] + [in_vmem] * 5,
        out_specs=[in_vmem, in_vmem],
        scratch_shapes=[
            VMEM((3, count, size), F32),
            VMEM((3, slots, each, size), F32),
            VMEM((3, slots, each, size), F32),
            VMEM((3, hangs, size), F32),
            VMEM((3, hangs, size), F32),
            VMEM((2, hangs), jnp.int32),
            pltpu.SMEM((2, hangs), jnp.int32),
            VMEM((1, size), F32),
            VMEM((group - 1, 1, size), F32),
            VMEM((depth - 1, 1, size), F32),
            sem((3, slots)), sem((3, slots)), sem((3,)), sem((3,)), sem((3,)), sem, sem, sem, sem,
        ],
        compiler_params=pltpu.CompilerParams(collective_id=0, has_side_effects=True),
    )(
        share_map[0], blocks, share_map.reshape(1, -1), jnp.transpose(hang_parent[0]), hang_child, energy_part,
    )
    scale = 0.5 / (width * elements * ranks * levels)
    return projected, energy[0, 0] * F32(scale)


def solution(mesh):
    both = ("dom", "level")
    placed = (
        P(both, None), P(), P(), P(both), P(both), P(both), P(None, both),
        P(both, None, None), P(both, None), P(both, None, None),
    )
    return jax.shard_map(
        shards, mesh=mesh, in_specs=placed, out_specs=(P(None, both, None), P()), check_vma=False
    )
```

```python
import jax
import jax.numpy as jnp
from jax import lax
from jax.experimental import pallas as pl
from jax.experimental.pallas import tpu as pltpu
from jax.sharding import PartitionSpec as P

MESH = pl.DeviceIdType.MESH
VMEM = pltpu.VMEM
F32 = jnp.float32
BF16 = jnp.bfloat16
CHUNK = 256
LOADS = 6
TILE = 256
PLANES = 16


def split(x):
    high = x.astype(BF16)
    low = (x - high.astype(F32)).astype(BF16)
    return jnp.concatenate([high, low], axis=1)


def one_hot(base, rows, ids):
    near = ids - base
    row = lax.broadcasted_iota(jnp.int32, (rows, ids.shape[1]), 0)
    return (row == near).astype(F32).astype(BF16)


def kernel(
    live, values_h, stiff_mu_h, stiff_lam_h, mu_h, lam_h, ids_h, share_h, parents_h, children_h,
    out, energy,
    values, stiff, mu, lam, ids, share, slots_v, parents, children, terms,
    gather, arrived, child_out, child_in, wanted_in, wanted, spark, column, plane_sum, plane,
    small_sem, stiff_sem, value_sem, share_send, share_recv, child_send, child_recv, wanted_sem,
    column_send, column_recv, plane_send, plane_recv,
):
    dom, level = lax.axis_index("dom"), lax.axis_index("level")
    ranks, levels = lax.axis_size("dom"), lax.axis_size("level")
    elements, width = values.shape
    size = width // 3
    count = out.shape[1]
    slots, each = share.shape
    half = slots // 2

    small = [
        pltpu.make_async_copy(src, dst, small_sem.at[i])
        for i, (src, dst) in enumerate(
            [
                (mu_h, mu), (lam_h, lam), (ids_h, ids), (share_h, share), (share_h, slots_v),
                (parents_h, parents), (children_h, children),
            ]
        )
    ]
    stiffs = []
    for c in range(3):
        for k, src in enumerate((stiff_mu_h, stiff_lam_h)):
            stiffs.append(
                pltpu.make_async_copy(
                    src.at[:, pl.ds(c * size, size)], stiff.at[c, :, pl.ds(k * size, size)], stiff_sem.at[c, k]
                )
            )
    step = elements // LOADS
    loads = [
        pltpu.make_async_copy(
            values_h.at[pl.ds(i * step, step), :], values.at[pl.ds(i * step, step), :], value_sem.at[i]
        )
        for i in range(LOADS)
    ]
    for copy in small[:2] + stiffs + loads + small[2:]:
        copy.start()

    offsets = [o + 1 for o in range(half)] + [-(o + 1) for o in range(half)]
    exists = [(dom + off >= 0) & (dom + off < ranks) for off in offsets]
    near = [(lax.rem(dom + off + ranks, ranks), level) for off in offsets]
    has_finer, has_coarser = level < levels - 1, level > 0
    finer = (dom, lax.rem(level + 1, levels))
    coarser = (dom, lax.rem(level + levels - 1, levels))
    slab = ranks // PLANES
    group = slab * levels
    place = lax.rem(dom, slab) * levels + level
    z = dom // slab
    in_column = [(lax.rem(z + k, PLANES) * slab + lax.rem(dom, slab), level) for k in range(1, PLANES)]
    in_plane = []
    for k in range(1, group):
        other = lax.rem(place + k, group)
        in_plane.append((z * slab + other // levels, lax.rem(other, levels)))

    barrier = pltpu.get_barrier_semaphore()

    def greet(device):
        pl.semaphore_signal(barrier, inc=1, device_id=device, device_id_type=MESH)

    greeted = jnp.int32(len(in_column) + len(in_plane))
    for device in in_column + in_plane:
        greet(device)
    for there, device in zip(exists + [has_finer, has_coarser], near + [finer, coarser]):
        pl.when(there)(lambda device=device: greet(device))
        greeted = greeted + there.astype(jnp.int32)

    def remote(src, dst, send, recv, device):
        return pltpu.make_async_remote_copy(
            src_ref=src, dst_ref=dst, send_sem=send, recv_sem=recv, device_id=device, device_id_type=MESH
        )

    for o in range(slots):
        @pl.when(jnp.logical_not(exists[o]))
        def _():
            arrived[:, (o) * each : (o + 1) * each, :] = jnp.zeros((3, each, size), F32)

    @pl.when(jnp.logical_not(has_coarser))
    def _():
        child_in[...] = jnp.zeros(child_in.shape, F32)

    for copy in small[:2]:
        copy.wait()
    at_row = lax.broadcasted_iota(jnp.int32, mu.shape, 0) * 128
    at_row = at_row + lax.broadcasted_iota(jnp.int32, mu.shape, 1)
    alive = at_row < live[0]
    mu_t = jnp.transpose(jnp.where(alive, mu[...], 0.0))
    lam_t = jnp.transpose(jnp.where(alive, lam[...], 0.0))
    for copy in stiffs:
        copy.wait()
    total = jnp.zeros((8, size), F32)
    n = CHUNK // 128
    for g in range(elements // CHUNK):
        if (g * CHUNK) % step == 0:
            loads[g * CHUNK // step].wait()
        rows = pl.ds(g * CHUNK, CHUNK)
        part = values[rows, :]
        a = jnp.concatenate([mu_t[:, g * n + i : g * n + i + 1] for i in range(n)], axis=0)
        b = jnp.concatenate([lam_t[:, g * n + i : g * n + i + 1] for i in range(n)], axis=0)
        for c in range(3):
            both = jnp.dot(part, stiff[c], preferred_element_type=F32)
            forces = a * both[:, :size] + b * both[:, size:]
            work = part[:, c * size : (c + 1) * size].astype(F32) * forces
            total = total + jnp.sum(work.reshape(CHUNK // 8, 8, size), axis=0)
            terms[c, rows, :] = split(forces)
    spark[...] = jnp.sum(total, axis=0, keepdims=True)
    for copy in small[2:]:
        copy.wait()

    pl.semaphore_wait(barrier, greeted)
    column_copies = [
        remote(spark, column.at[k], column_send, column_recv, device) for k, device in enumerate(in_column)
    ]
    for copy in column_copies:
        copy.start()
    ask = remote(parents, wanted_in, wanted_sem.at[0], wanted_sem.at[1], coarser)
    pl.when(has_coarser)(ask.start)

    shares = []
    for c in range(3):
        def tile(i, carry):
            base = pl.multiple_of(i * TILE, TILE)
            hot = one_hot(base, TILE, ids[c : c + 1, :])
            both = jnp.dot(hot, terms[c], preferred_element_type=F32)
            out[c, pl.ds(base, TILE), :] = both[:, :size] + both[:, size:]
            return carry

        lax.fori_loop(0, count // TILE, tile, 0)

        for o in range(slots):
            def pick(s, carry):
                row = jnp.minimum(share[o, s], count - 1)
                gather[c, pl.ds(o * each + s, 1), :] = out[c, pl.ds(row, 1), :]
                return carry

            lax.fori_loop(0, each, pick, 0, unroll=True)
        for o in range(slots):
            opposite = (o + half) % slots
            copy = remote(
                gather.at[c, pl.ds(o * each, each), :], arrived.at[c, pl.ds(opposite * each, each), :],
                share_send.at[c, o], share_recv.at[c, opposite], near[o],
            )
            pl.when(exists[o])(copy.start)
            shares.append(copy)

    @pl.when(has_finer)
    def _():
        ask.wait_recv()
        fetch = pltpu.make_async_copy(wanted_in, wanted, wanted_sem.at[2])
        fetch.start()
        fetch.wait()

    slot_ids = jnp.concatenate([slots_v[o : o + 1, :] for o in range(slots)], axis=1)
    hot = one_hot(0, count, slot_ids)
    sent = []
    for c in range(3):
        for o in range(slots):
            back = remote(
                gather.at[c, pl.ds(o * each, each), :], arrived.at[c, pl.ds(o * each, each), :],
                share_send.at[c, o], share_recv.at[c, o], near[o],
            )
            pl.when(exists[o])(back.wait_recv)
        both = jnp.dot(hot, split(arrived[c]), preferred_element_type=F32)
        out[c] = out[c] + (both[:, :size] + both[:, size:])
        copy = remote(child_out.at[c], child_in.at[c], child_send.at[c], child_recv.at[c], finer)
        sent.append(copy)

        @pl.when(has_finer)
        def _():
            def pair(h, carry):
                one = out[c, pl.ds(wanted[0, h], 1), :]
                two = out[c, pl.ds(wanted[1, h], 1), :]
                child_out[c, pl.ds(h, 1), :] = 0.5 * (one + two)
                return carry

            lax.fori_loop(0, wanted.shape[1], pair, 0, unroll=True)
            copy.start()

    hangs = one_hot(0, count, children[...])
    keep = 1.0 - jnp.sum(hangs.astype(F32), axis=1, keepdims=True)
    for c in range(3):
        pl.when(has_coarser)(sent[c].wait_recv)
        both = jnp.dot(hangs, split(child_in[c]), preferred_element_type=F32)
        out[c] = keep * out[c] + (both[:, :size] + both[:, size:])

    remote(column, column, column_send, column_recv, finer).wait_recv()
    plane_sum[...] = spark[...] + jnp.sum(column[...], axis=0)
    plane_copies = [
        remote(plane_sum, plane.at[k], plane_send, plane_recv, device) for k, device in enumerate(in_plane)
    ]
    for copy in plane_copies:
        copy.start()
    for copy in column_copies:
        copy.wait_send()
    for c in range(3):
        for o in range(slots):
            pl.when(exists[o])(shares[c * slots + o].wait_send)
        pl.when(has_finer)(sent[c].wait_send)
    pl.when(has_coarser)(ask.wait_send)
    remote(plane, plane, plane_send, plane_recv, finer).wait_recv()
    everything = plane_sum[...] + jnp.sum(plane[...], axis=0)
    scale = 0.5 / (width * elements * ranks * levels)
    energy[...] = jnp.sum(everything, axis=1, keepdims=True) * scale
    for copy in plane_copies:
        copy.wait_send()


def shards(
    dg_values, stiff_mu, stiff_lam, coef_mu, coef_lam, elem_count, elem_block, share_map, hang_child, hang_parent
):
    elements, width = dg_values.shape
    size = width // 3
    count = elements // 3
    slots, each = share_map.shape[1:]
    hangs = hang_child.shape[1]
    group = lax.axis_size("dom") // PLANES * lax.axis_size("level")
    rows = elements // 128
    in_hbm = pl.BlockSpec(memory_space=pltpu.HBM)
    in_vmem = pl.BlockSpec(memory_space=VMEM)
    sem = pltpu.SemaphoreType.DMA
    i32 = jnp.int32
    projected, energy = pl.pallas_call(
        kernel,
        out_shape=[jax.ShapeDtypeStruct((3, count, size), F32), jax.ShapeDtypeStruct((1, 1), F32)],
        in_specs=[pl.BlockSpec(memory_space=pltpu.SMEM)] + [in_hbm] * 9,
        out_specs=[in_vmem, in_vmem],
        scratch_shapes=[
            VMEM((elements, width), BF16),
            VMEM((3, width, 2 * size), BF16),
            VMEM((rows, 128), F32),
            VMEM((rows, 128), F32),
            VMEM((3, elements), i32),
            pltpu.SMEM((slots, each), i32),
            VMEM((slots, each), i32),
            VMEM((2, hangs), i32),
            VMEM((1, hangs), i32),
            VMEM((3, elements, 2 * size), BF16),
            VMEM((3, slots * each, size), F32),
            VMEM((3, slots * each, size), F32),
            VMEM((3, hangs, size), F32),
            VMEM((3, hangs, size), F32),
            VMEM((2, hangs), i32),
            pltpu.SMEM((2, hangs), i32),
            VMEM((1, size), F32),
            VMEM((PLANES - 1, 1, size), F32),
            VMEM((1, size), F32),
            VMEM((group - 1, 1, size), F32),
            sem((7,)), sem((3, 2)), sem((LOADS,)), sem((3, slots)), sem((3, slots)), sem((3,)), sem((3,)), sem((3,)),
            sem, sem, sem, sem,
        ],
        compiler_params=pltpu.CompilerParams(
            collective_id=0, has_side_effects=True, vmem_limit_bytes=24 * 2**20
        ),
    )(
        elem_count,
        *(
            pltpu.with_memory_space_constraint(x, pltpu.HBM)
            for x in (
                dg_values, stiff_mu, stiff_lam, coef_mu.reshape(rows, 128), coef_lam.reshape(rows, 128),
                elem_block, share_map[0], jnp.transpose(hang_parent[0]), hang_child,
            )
        ),
    )
    return projected, energy[0, 0]


def solution(mesh):
    both = ("dom", "level")
    placed = (
        P(both, None), P(), P(), P(both), P(both), P(both), P(None, both),
        P(both, None, None), P(both, None), P(both, None, None),
    )
    return jax.shard_map(
        shards, mesh=mesh, in_specs=placed, out_specs=(P(None, both, None), P()), check_vma=False
    )
```

```python
import jax
import jax.numpy as jnp
from jax import lax
from jax.experimental import pallas as pl
from jax.experimental.pallas import tpu as pltpu
from jax.sharding import PartitionSpec as P

MESH = pl.DeviceIdType.MESH
VMEM = pltpu.VMEM
F32 = jnp.float32
BF16 = jnp.bfloat16
CHUNK = 256
LOADS = 6
TILE = 256
PLANES = 16
FIRST = 6


def split(x):
    high = x.astype(BF16)
    low = (x - high.astype(F32)).astype(BF16)
    return jnp.concatenate([high, low], axis=1)


def one_hot(base, rows, ids):
    near = ids - base
    row = lax.broadcasted_iota(jnp.int32, (rows, ids.shape[1]), 0)
    return (row == near).astype(F32).astype(BF16)


def kernel(
    live, values_h, stiff_mu_h, stiff_lam_h, mu_h, lam_h, ids_h, share_h, parents_h, children_h,
    out, energy,
    values, stiff, mu, lam, ids, share, slots_v, parents, children, terms,
    gather, arrived, child_out, child_in, wanted_in, wanted, spark, column, plane_sum, plane,
    small_sem, stiff_sem, value_sem, share_send, share_recv, child_send, child_recv, wanted_sem,
    column_send, column_recv, plane_send, plane_recv,
):
    dom, level = lax.axis_index("dom"), lax.axis_index("level")
    ranks, levels = lax.axis_size("dom"), lax.axis_size("level")
    elements, width = values.shape
    size = width // 3
    count = out.shape[1]
    slots, each = share.shape
    half = slots // 2

    small = [
        pltpu.make_async_copy(src, dst, small_sem.at[i])
        for i, (src, dst) in enumerate(
            [
                (mu_h, mu), (lam_h, lam), (ids_h, ids), (share_h, share), (share_h, slots_v),
                (parents_h, parents), (children_h, children),
            ]
        )
    ]
    stiffs = [
        pltpu.make_async_copy(src, stiff.at[k], stiff_sem.at[k]) for k, src in enumerate((stiff_mu_h, stiff_lam_h))
    ]
    step = elements // LOADS
    loads = [
        pltpu.make_async_copy(
            values_h.at[pl.ds(i * step, step), :], values.at[pl.ds(i * step, step), :], value_sem.at[i]
        )
        for i in range(LOADS)
    ]
    for copy in small[:2] + stiffs + loads + small[2:]:
        copy.start()

    offsets = [o + 1 for o in range(half)] + [-(o + 1) for o in range(half)]
    exists = [(dom + off >= 0) & (dom + off < ranks) for off in offsets]
    near = [(lax.rem(dom + off + ranks, ranks), level) for off in offsets]
    has_finer, has_coarser = level < levels - 1, level > 0
    finer = (dom, lax.rem(level + 1, levels))
    coarser = (dom, lax.rem(level + levels - 1, levels))
    slab = ranks // PLANES
    group = slab * levels
    place = lax.rem(dom, slab) * levels + level
    z = dom // slab
    in_column = [(lax.rem(z + k, PLANES) * slab + lax.rem(dom, slab), level) for k in range(1, PLANES)]
    in_plane = []
    for k in range(1, group):
        other = lax.rem(place + k, group)
        in_plane.append((z * slab + other // levels, lax.rem(other, levels)))

    barrier = pltpu.get_barrier_semaphore()

    def greet(device):
        pl.semaphore_signal(barrier, inc=1, device_id=device, device_id_type=MESH)

    greeted = jnp.int32(len(in_column) + len(in_plane))
    for device in in_column + in_plane:
        greet(device)
    for there, device in zip(exists + [has_finer, has_coarser], near + [finer, coarser]):
        pl.when(there)(lambda device=device: greet(device))
        greeted = greeted + there.astype(jnp.int32)

    def remote(src, dst, send, recv, device):
        return pltpu.make_async_remote_copy(
            src_ref=src, dst_ref=dst, send_sem=send, recv_sem=recv, device_id=device, device_id_type=MESH
        )

    for o in range(slots):
        @pl.when(jnp.logical_not(exists[o]))
        def _():
            arrived[:, (o) * each : (o + 1) * each, :] = jnp.zeros((3, each, size), F32)

    @pl.when(jnp.logical_not(has_coarser))
    def _():
        child_in[...] = jnp.zeros(child_in.shape, F32)

    for copy in small[:2]:
        copy.wait()
    at_row = lax.broadcasted_iota(jnp.int32, mu.shape, 0) * 128
    at_row = at_row + lax.broadcasted_iota(jnp.int32, mu.shape, 1)
    alive = at_row < live[0]
    mu_t = jnp.transpose(jnp.where(alive, mu[...], 0.0))
    lam_t = jnp.transpose(jnp.where(alive, lam[...], 0.0))
    for copy in stiffs:
        copy.wait()
    total = jnp.zeros((8, size), F32)
    n = CHUNK // 128
    for g in range(elements // CHUNK):
        if (g * CHUNK) % step == 0:
            loads[g * CHUNK // step].wait()
        rows = pl.ds(g * CHUNK, CHUNK)
        part = values[rows, :]
        a = jnp.concatenate([mu_t[:, g * n + i : g * n + i + 1] for i in range(n)], axis=0)
        b = jnp.concatenate([lam_t[:, g * n + i : g * n + i + 1] for i in range(n)], axis=0)
        for c in range(3):
            cols = slice(c * size, (c + 1) * size)
            pair = jnp.concatenate([stiff[0, :, cols], stiff[1, :, cols]], axis=1)
            both = jnp.dot(part, pair, preferred_element_type=F32)
            forces = a * both[:, :size] + b * both[:, size:]
            work = part[:, cols].astype(F32) * forces
            total = total + jnp.sum(work.reshape(CHUNK // 8, 8, size), axis=0)
            terms[c, rows, :] = split(forces)
    spark[...] = jnp.sum(total, axis=0, keepdims=True)
    for copy in small[2:]:
        copy.wait()

    column_copies = [
        remote(spark, column.at[k], column_send, column_recv, device) for k, device in enumerate(in_column)
    ]
    ask = remote(parents, wanted_in, wanted_sem.at[0], wanted_sem.at[1], coarser)
    shares = []
    for c in range(3):
        for o in range(slots):
            opposite = (o + half) % slots
            shares.append(
                remote(
                    gather.at[c, pl.ds(o * each, each), :], arrived.at[c, pl.ds(opposite * each, each), :],
                    share_send.at[c, o], share_recv.at[c, opposite], near[o],
                )
            )

    def meet():
        pl.semaphore_wait(barrier, greeted)
        for copy in column_copies:
            copy.start()
        pl.when(has_coarser)(ask.start)

    def send_shares(c):
        for o in range(slots):
            pl.when(exists[o])(shares[c * slots + o].start)

    soon = z >= FIRST
    pl.when(soon)(meet)

    def sums(c):
        for i in range(count // TILE):
            hot = one_hot(i * TILE, TILE, ids[c : c + 1, :])
            both = jnp.dot(hot, terms[c], preferred_element_type=F32)
            out[c, i * TILE : (i + 1) * TILE, :] = both[:, :size] + both[:, size:]

    def pick(c):
        for o in range(slots):
            for s in range(each):
                row = jnp.minimum(share[o, s], count - 1)
                gather[c, o * each + s : o * each + s + 1, :] = out[c, pl.ds(row, 1), :]

    sums(0)
    pick(0)
    sums(1)
    pl.when(soon)(lambda: send_shares(0))
    pick(1)
    sums(2)
    pl.when(soon)(lambda: send_shares(1))
    pick(2)
    pl.when(soon)(lambda: send_shares(2))

    @pl.when(jnp.logical_not(soon))
    def _():
        meet()
        for c in range(3):
            send_shares(c)

    @pl.when(has_finer)
    def _():
        ask.wait_recv()
        fetch = pltpu.make_async_copy(wanted_in, wanted, wanted_sem.at[2])
        fetch.start()
        fetch.wait()

    slot_ids = jnp.concatenate([slots_v[o : o + 1, :] for o in range(slots)], axis=1)
    hot = one_hot(0, count, slot_ids)
    sent = []
    for c in range(3):
        for o in range(slots):
            back = remote(
                gather.at[c, pl.ds(o * each, each), :], arrived.at[c, pl.ds(o * each, each), :],
                share_send.at[c, o], share_recv.at[c, o], near[o],
            )
            pl.when(exists[o])(back.wait_recv)
        both = jnp.dot(hot, split(arrived[c]), preferred_element_type=F32)
        out[c] = out[c] + (both[:, :size] + both[:, size:])
        copy = remote(child_out.at[c], child_in.at[c], child_send.at[c], child_recv.at[c], finer)
        sent.append(copy)

        @pl.when(has_finer)
        def _():
            def pair(h, carry):
                one = out[c, pl.ds(wanted[0, h], 1), :]
                two = out[c, pl.ds(wanted[1, h], 1), :]
                child_out[c, pl.ds(h, 1), :] = 0.5 * (one + two)
                return carry

            lax.fori_loop(0, wanted.shape[1], pair, 0, unroll=True)
            copy.start()

    hangs = one_hot(0, count, children[...])
    keep = 1.0 - jnp.sum(hangs.astype(F32), axis=1, keepdims=True)
    for c in range(3):
        pl.when(has_coarser)(sent[c].wait_recv)
        both = jnp.dot(hangs, split(child_in[c]), preferred_element_type=F32)
        out[c] = keep * out[c] + (both[:, :size] + both[:, size:])

    remote(column, column, column_send, column_recv, finer).wait_recv()
    plane_sum[...] = spark[...] + jnp.sum(column[...], axis=0)
    plane_copies = [
        remote(plane_sum, plane.at[k], plane_send, plane_recv, device) for k, device in enumerate(in_plane)
    ]
    for copy in plane_copies:
        copy.start()
    for copy in column_copies:
        copy.wait_send()
    for c in range(3):
        for o in range(slots):
            pl.when(exists[o])(shares[c * slots + o].wait_send)
        pl.when(has_finer)(sent[c].wait_send)
    pl.when(has_coarser)(ask.wait_send)
    remote(plane, plane, plane_send, plane_recv, finer).wait_recv()
    everything = plane_sum[...] + jnp.sum(plane[...], axis=0)
    scale = 0.5 / (width * elements * ranks * levels)
    energy[...] = jnp.sum(everything, axis=1, keepdims=True) * scale
    for copy in plane_copies:
        copy.wait_send()


def shards(
    dg_values, stiff_mu, stiff_lam, coef_mu, coef_lam, elem_count, elem_block, share_map, hang_child, hang_parent
):
    elements, width = dg_values.shape
    size = width // 3
    count = elements // 3
    slots, each = share_map.shape[1:]
    hangs = hang_child.shape[1]
    group = lax.axis_size("dom") // PLANES * lax.axis_size("level")
    rows = elements // 128
    in_hbm = pl.BlockSpec(memory_space=pltpu.HBM)
    in_vmem = pl.BlockSpec(memory_space=VMEM)
    sem = pltpu.SemaphoreType.DMA
    i32 = jnp.int32
    projected, energy = pl.pallas_call(
        kernel,
        out_shape=[jax.ShapeDtypeStruct((3, count, size), F32), jax.ShapeDtypeStruct((1, 1), F32)],
        in_specs=[pl.BlockSpec(memory_space=pltpu.SMEM)] + [in_hbm] * 9,
        out_specs=[in_vmem, in_vmem],
        scratch_shapes=[
            VMEM((elements, width), BF16),
            VMEM((2, width, width), BF16),
            VMEM((rows, 128), F32),
            VMEM((rows, 128), F32),
            VMEM((3, elements), i32),
            pltpu.SMEM((slots, each), i32),
            VMEM((slots, each), i32),
            VMEM((2, hangs), i32),
            VMEM((1, hangs), i32),
            VMEM((3, elements, 2 * size), BF16),
            VMEM((3, slots * each, size), F32),
            VMEM((3, slots * each, size), F32),
            VMEM((3, hangs, size), F32),
            VMEM((3, hangs, size), F32),
            VMEM((2, hangs), i32),
            pltpu.SMEM((2, hangs), i32),
            VMEM((1, size), F32),
            VMEM((PLANES - 1, 1, size), F32),
            VMEM((1, size), F32),
            VMEM((group - 1, 1, size), F32),
            sem((7,)), sem((2,)), sem((LOADS,)), sem((3, slots)), sem((3, slots)), sem((3,)), sem((3,)), sem((3,)),
            sem, sem, sem, sem,
        ],
        compiler_params=pltpu.CompilerParams(
            collective_id=0, has_side_effects=True, vmem_limit_bytes=24 * 2**20
        ),
    )(
        elem_count,
        *(
            pltpu.with_memory_space_constraint(x, pltpu.HBM)
            for x in (
                dg_values, stiff_mu, stiff_lam, coef_mu.reshape(rows, 128), coef_lam.reshape(rows, 128),
                elem_block, share_map[0], jnp.transpose(hang_parent[0]), hang_child,
            )
        ),
    )
    return projected, energy[0, 0]


def solution(mesh):
    both = ("dom", "level")
    placed = (
        P(both, None), P(), P(), P(both), P(both), P(both), P(None, both),
        P(both, None, None), P(both, None), P(both, None, None),
    )
    return jax.shard_map(
        shards, mesh=mesh, in_specs=placed, out_specs=(P(None, both, None), P()), check_vma=False
    )
```

```python
import jax
import jax.numpy as jnp
from jax import lax
from jax.experimental import pallas as pl
from jax.experimental.pallas import tpu as pltpu
from jax.sharding import PartitionSpec as P

MESH = pl.DeviceIdType.MESH
VMEM = pltpu.VMEM
F32 = jnp.float32
BF16 = jnp.bfloat16
CHUNK = 256
LOADS = 6
TILE = 256
PLANES = 16
FIRST = 6
EARLY = 3


def split(x):
    high = x.astype(BF16)
    low = (x - high.astype(F32)).astype(BF16)
    return jnp.concatenate([high, low], axis=1)


def one_hot(base, rows, ids):
    near = ids - base
    row = lax.broadcasted_iota(jnp.int32, (rows, ids.shape[1]), 0)
    return (row == near).astype(F32).astype(BF16)


def kernel(
    live_h, values_h, stiff_mu_h, stiff_lam_h, mu_h, lam_h, ids_h, share_h, parents_h, children_h,
    out, energy,
    live, values, stiff, mu, lam, ids, share, slots_v, parents, children, terms,
    gather, arrived, child_out, child_in, wanted_in, wanted, hot, hangs, keep, spark, column, plane_sum, plane,
    small_sem, stiff_sem, value_sem, share_send, share_recv, child_send, child_recv, wanted_sem,
    column_send, column_recv, plane_send, plane_recv,
):
    dom, level = lax.axis_index("dom"), lax.axis_index("level")
    ranks, levels = lax.axis_size("dom"), lax.axis_size("level")
    elements, width = values.shape
    size = width // 3
    count = out.shape[1]
    slots, each = share.shape
    half = slots // 2

    small = [
        pltpu.make_async_copy(src, dst, small_sem.at[i])
        for i, (src, dst) in enumerate(
            [
                (live_h, live), (mu_h, mu), (lam_h, lam), (ids_h, ids), (share_h, share), (share_h, slots_v),
                (parents_h, parents), (children_h, children),
            ]
        )
    ]
    stiffs = [
        pltpu.make_async_copy(src, stiff.at[k], stiff_sem.at[k]) for k, src in enumerate((stiff_mu_h, stiff_lam_h))
    ]
    step = elements // LOADS
    loads = [
        pltpu.make_async_copy(
            values_h.at[pl.ds(i * step, step), :], values.at[pl.ds(i * step, step), :], value_sem.at[i]
        )
        for i in range(LOADS)
    ]
    for copy in small[:3] + stiffs + loads + small[3:]:
        copy.start()

    offsets = [o + 1 for o in range(half)] + [-(o + 1) for o in range(half)]
    exists = [(dom + off >= 0) & (dom + off < ranks) for off in offsets]
    near = [(lax.rem(dom + off + ranks, ranks), level) for off in offsets]
    has_finer, has_coarser = level < levels - 1, level > 0
    finer = (dom, lax.rem(level + 1, levels))
    coarser = (dom, lax.rem(level + levels - 1, levels))
    slab = ranks // PLANES
    group = slab * levels
    place = lax.rem(dom, slab) * levels + level
    z = dom // slab
    steps = sorted(range(1, PLANES), key=lambda k: abs(k - PLANES // 2))
    in_column = [(lax.rem(z + k, PLANES) * slab + lax.rem(dom, slab), level) for k in steps]
    in_plane = []
    for k in range(1, group):
        other = lax.rem(place + k, group)
        in_plane.append((z * slab + other // levels, lax.rem(other, levels)))

    barrier = pltpu.get_barrier_semaphore()

    def greet(device):
        pl.semaphore_signal(barrier, inc=1, device_id=device, device_id_type=MESH)

    early = z < EARLY
    ahead = [lax.rem(z + k, PLANES) < EARLY for k in steps]
    for device in in_plane:
        greet(device)
    for other, device in zip(ahead, in_column):
        pl.when(early == other)(lambda device=device: greet(device))
    greeted = jnp.int32(len(in_plane)) + jnp.where(early, EARLY - 1, PLANES - 1)
    for there, device in zip(exists + [has_finer, has_coarser], near + [finer, coarser]):
        pl.when(there)(lambda device=device: greet(device))
        greeted = greeted + there.astype(jnp.int32)

    def remote(src, dst, send, recv, device):
        return pltpu.make_async_remote_copy(
            src_ref=src, dst_ref=dst, send_sem=send, recv_sem=recv, device_id=device, device_id_type=MESH
        )

    for o in range(slots):
        @pl.when(jnp.logical_not(exists[o]))
        def _():
            arrived[:, (o) * each : (o + 1) * each, :] = jnp.zeros((3, each, size), F32)

    @pl.when(jnp.logical_not(has_coarser))
    def _():
        child_in[...] = jnp.zeros(child_in.shape, F32)

    for copy in small[:3]:
        copy.wait()
    at_row = lax.broadcasted_iota(jnp.int32, mu.shape, 0) * 128
    at_row = at_row + lax.broadcasted_iota(jnp.int32, mu.shape, 1)
    alive = at_row < live[0, 0]
    mu_t = jnp.transpose(jnp.where(alive, mu[...], 0.0))
    lam_t = jnp.transpose(jnp.where(alive, lam[...], 0.0))
    for copy in stiffs:
        copy.wait()
    total = jnp.zeros((8, size), F32)
    n = CHUNK // 128
    for g in range(elements // CHUNK):
        if (g * CHUNK) % step == 0:
            loads[g * CHUNK // step].wait()
        rows = pl.ds(g * CHUNK, CHUNK)
        part = values[rows, :]
        a = jnp.concatenate([mu_t[:, g * n + i : g * n + i + 1] for i in range(n)], axis=0)
        b = jnp.concatenate([lam_t[:, g * n + i : g * n + i + 1] for i in range(n)], axis=0)
        for c in range(3):
            cols = slice(c * size, (c + 1) * size)
            pair = jnp.concatenate([stiff[0, :, cols], stiff[1, :, cols]], axis=1)
            both = jnp.dot(part, pair, preferred_element_type=F32)
            forces = a * both[:, :size] + b * both[:, size:]
            work = part[:, cols].astype(F32) * forces
            total = total + jnp.sum(work.reshape(CHUNK // 8, 8, size), axis=0)
            terms[c, rows, :] = split(forces)
    spark[...] = jnp.sum(total, axis=0, keepdims=True)
    for copy in small[3:]:
        copy.wait()

    column_copies = [
        remote(spark, column.at[k], column_send, column_recv, device) for k, device in enumerate(in_column)
    ]
    ask = remote(parents, wanted_in, wanted_sem.at[0], wanted_sem.at[1], coarser)
    shares = []
    for c in range(3):
        for o in range(slots):
            opposite = (o + half) % slots
            shares.append(
                remote(
                    gather.at[c, pl.ds(o * each, each), :], arrived.at[c, pl.ds(opposite * each, each), :],
                    share_send.at[c, o], share_recv.at[c, opposite], near[o],
                )
            )

    def meet():
        pl.semaphore_wait(barrier, greeted)
        for other, copy in zip(ahead, column_copies):
            pl.when(jnp.logical_not(early) | other)(copy.start)
        for other, device in zip(ahead, in_column):
            pl.when(early != other)(lambda device=device: greet(device))
        pl.when(has_coarser)(ask.start)

    def meet_far():
        pl.semaphore_wait(barrier, PLANES - EARLY)
        for other, copy in zip(ahead, column_copies):
            pl.when(jnp.logical_not(other))(copy.start)

    def send_shares(c):
        for o in range(slots):
            pl.when(exists[o])(shares[c * slots + o].start)

    plane_copies = [
        remote(plane_sum, plane.at[k], plane_send, plane_recv, device) for k, device in enumerate(in_plane)
    ]

    def pass_energy():
        remote(column, column, column_send, column_recv, finer).wait_recv()
        plane_sum[...] = spark[...] + jnp.sum(column[...], axis=0)
        for copy in plane_copies:
            copy.start()

    soon = early | (z >= FIRST)
    pl.when(soon)(meet)

    def sums(c):
        for i in range(count // TILE):
            hot = one_hot(i * TILE, TILE, ids[c : c + 1, :])
            both = jnp.dot(hot, terms[c], preferred_element_type=F32)
            out[c, i * TILE : (i + 1) * TILE, :] = both[:, :size] + both[:, size:]

    def pick(c):
        for o in range(slots):
            for s in range(each):
                row = jnp.minimum(share[o, s], count - 1)
                gather[c, o * each + s : o * each + s + 1, :] = out[c, pl.ds(row, 1), :]

    sums(0)
    pick(0)
    sums(1)
    pl.when(soon)(lambda: send_shares(0))
    pick(1)
    sums(2)
    pl.when(soon)(lambda: send_shares(1))
    pick(2)
    pl.when(soon)(lambda: send_shares(2))

    slot_ids = jnp.concatenate([slots_v[o : o + 1, :] for o in range(slots)], axis=1)
    hot[...] = one_hot(0, count, slot_ids)
    chosen = one_hot(0, count, children[...])
    hangs[...] = chosen
    keep[...] = jnp.broadcast_to(1.0 - jnp.sum(chosen.astype(F32), axis=1, keepdims=True), keep.shape)

    @pl.when(jnp.logical_not(soon))
    def _():
        meet()
        for c in range(3):
            send_shares(c)

    @pl.when(has_finer)
    def _():
        ask.wait_recv()
        fetch = pltpu.make_async_copy(wanted_in, wanted, wanted_sem.at[2])
        fetch.start()
        fetch.wait()

    sent = []
    for c in range(3):
        for o in range(slots):
            back = remote(
                gather.at[c, pl.ds(o * each, each), :], arrived.at[c, pl.ds(o * each, each), :],
                share_send.at[c, o], share_recv.at[c, o], near[o],
            )
            pl.when(exists[o])(back.wait_recv)
        both = jnp.dot(hot[...], split(arrived[c]), preferred_element_type=F32)
        out[c] = out[c] + (both[:, :size] + both[:, size:])
        copy = remote(child_out.at[c], child_in.at[c], child_send.at[c], child_recv.at[c], finer)
        sent.append(copy)

        @pl.when(has_finer)
        def _():
            def pair(h, carry):
                one = out[c, pl.ds(wanted[0, h], 1), :]
                two = out[c, pl.ds(wanted[1, h], 1), :]
                child_out[c, pl.ds(h, 1), :] = 0.5 * (one + two)
                return carry

            lax.fori_loop(0, wanted.shape[1], pair, 0, unroll=True)
            copy.start()

    pl.when(early)(meet_far)
    pass_energy()

    for c in range(3):
        pl.when(has_coarser)(sent[c].wait_recv)
        both = jnp.dot(hangs[...], split(child_in[c]), preferred_element_type=F32)
        out[c] = keep[...] * out[c] + (both[:, :size] + both[:, size:])

    for copy in column_copies:
        copy.wait_send()
    for c in range(3):
        for o in range(slots):
            pl.when(exists[o])(shares[c * slots + o].wait_send)
        pl.when(has_finer)(sent[c].wait_send)
    pl.when(has_coarser)(ask.wait_send)
    remote(plane, plane, plane_send, plane_recv, finer).wait_recv()
    everything = plane_sum[...] + jnp.sum(plane[...], axis=0)
    scale = 0.5 / (width * elements * ranks * levels)
    energy[...] = jnp.sum(everything, axis=1, keepdims=True) * scale
    for copy in plane_copies:
        copy.wait_send()


def shards(
    dg_values, stiff_mu, stiff_lam, coef_mu, coef_lam, elem_count, elem_block, share_map, hang_child, hang_parent
):
    elements, width = dg_values.shape
    size = width // 3
    count = elements // 3
    slots, each = share_map.shape[1:]
    hangs = hang_child.shape[1]
    group = lax.axis_size("dom") // PLANES * lax.axis_size("level")
    rows = elements // 128
    in_hbm = pl.BlockSpec(memory_space=pltpu.HBM)
    in_vmem = pl.BlockSpec(memory_space=VMEM)
    sem = pltpu.SemaphoreType.DMA
    i32 = jnp.int32
    projected, energy = pl.pallas_call(
        kernel,
        out_shape=[jax.ShapeDtypeStruct((3, count, size), F32), jax.ShapeDtypeStruct((1, 1), F32)],
        in_specs=[in_hbm] * 10,
        out_specs=[in_vmem, in_vmem],
        scratch_shapes=[
            pltpu.SMEM((1, 1), i32),
            VMEM((elements, width), BF16),
            VMEM((2, width, width), BF16),
            VMEM((rows, 128), F32),
            VMEM((rows, 128), F32),
            VMEM((3, elements), i32),
            pltpu.SMEM((slots, each), i32),
            VMEM((slots, each), i32),
            VMEM((2, hangs), i32),
            VMEM((1, hangs), i32),
            VMEM((3, elements, 2 * size), BF16),
            VMEM((3, slots * each, size), F32),
            VMEM((3, slots * each, size), F32),
            VMEM((3, hangs, size), F32),
            VMEM((3, hangs, size), F32),
            VMEM((2, hangs), i32),
            pltpu.SMEM((2, hangs), i32),
            VMEM((count, slots * each), BF16),
            VMEM((count, hangs), BF16),
            VMEM((count, size), F32),
            VMEM((1, size), F32),
            VMEM((PLANES - 1, 1, size), F32),
            VMEM((1, size), F32),
            VMEM((group - 1, 1, size), F32),
            sem((8,)), sem((2,)), sem((LOADS,)), sem((3, slots)), sem((3, slots)), sem((3,)), sem((3,)), sem((3,)),
            sem, sem, sem, sem,
        ],
        compiler_params=pltpu.CompilerParams(
            collective_id=0, has_side_effects=True, vmem_limit_bytes=24 * 2**20
        ),
    )(
        elem_count.reshape(1, 1),
        *(
            pltpu.with_memory_space_constraint(x, pltpu.HBM)
            for x in (
                dg_values, stiff_mu, stiff_lam, coef_mu.reshape(rows, 128), coef_lam.reshape(rows, 128),
                elem_block, share_map[0], jnp.transpose(hang_parent[0]), hang_child,
            )
        ),
    )
    return projected, energy[0, 0]


def solution(mesh):
    both = ("dom", "level")
    placed = (
        P(both, None), P(), P(), P(both), P(both), P(both), P(None, both),
        P(both, None, None), P(both, None), P(both, None, None),
    )
    return jax.shard_map(
        shards, mesh=mesh, in_specs=placed, out_specs=(P(None, both, None), P()), check_vma=False
    )
```

```python
import jax
import jax.numpy as jnp
from jax import lax
from jax.experimental import pallas as pl
from jax.experimental.pallas import tpu as pltpu
from jax.sharding import PartitionSpec as P

MESH = pl.DeviceIdType.MESH
VMEM = pltpu.VMEM
F32 = jnp.float32
BF16 = jnp.bfloat16
CHUNK = 256
LOADS = (4, 8)
TILE = 256
PLANES = 16
FIRST = 6
EARLY = 3


def split(x):
    high = x.astype(BF16)
    low = (x - high.astype(F32)).astype(BF16)
    return jnp.concatenate([high, low], axis=1)


def one_hot(base, rows, ids):
    near = ids - base
    row = lax.broadcasted_iota(jnp.int32, (rows, ids.shape[1]), 0)
    return (row == near).astype(F32).astype(BF16)


def kernel(
    live_h, values_h, stiff_mu_h, stiff_lam_h, mu_h, lam_h, ids_h, share_h, parents_h, children_h,
    out, energy,
    live, values, stiff, mu, lam, ids, share, slots_v, parents, children, terms,
    gather, arrived, child_out, child_in, wanted_in, wanted, hot, hangs, keep, spark, column, plane_sum, plane,
    small_sem, stiff_sem, value_sem, share_send, share_recv, child_send, child_recv, wanted_sem,
    column_send, column_recv, plane_send, plane_recv,
):
    dom, level = lax.axis_index("dom"), lax.axis_index("level")
    ranks, levels = lax.axis_size("dom"), lax.axis_size("level")
    elements, width = values.shape
    size = width // 3
    count = out.shape[1]
    slots, each = share.shape
    half = slots // 2

    small = [
        pltpu.make_async_copy(src, dst, small_sem.at[i])
        for i, (src, dst) in enumerate(
            [
                (live_h, live), (mu_h, mu), (lam_h, lam), (ids_h, ids), (share_h, share), (share_h, slots_v),
                (parents_h, parents), (children_h, children),
            ]
        )
    ]
    stiffs = [
        pltpu.make_async_copy(src, stiff.at[k], stiff_sem.at[k]) for k, src in enumerate((stiff_mu_h, stiff_lam_h))
    ]
    starts = [sum(LOADS[:i]) * CHUNK for i in range(len(LOADS))]
    loads = [
        pltpu.make_async_copy(
            values_h.at[pl.ds(start, n * CHUNK), :], values.at[pl.ds(start, n * CHUNK), :], value_sem.at[i]
        )
        for i, (start, n) in enumerate(zip(starts, LOADS))
    ]
    for copy in small[:3] + stiffs + loads + small[3:]:
        copy.start()

    offsets = [o + 1 for o in range(half)] + [-(o + 1) for o in range(half)]
    exists = [(dom + off >= 0) & (dom + off < ranks) for off in offsets]
    near = [(lax.rem(dom + off + ranks, ranks), level) for off in offsets]
    has_finer, has_coarser = level < levels - 1, level > 0
    finer = (dom, lax.rem(level + 1, levels))
    coarser = (dom, lax.rem(level + levels - 1, levels))
    slab = ranks // PLANES
    group = slab * levels
    place = lax.rem(dom, slab) * levels + level
    z = dom // slab
    steps = sorted(range(1, PLANES), key=lambda k: abs(k - PLANES // 2))
    in_column = [(lax.rem(z + k, PLANES) * slab + lax.rem(dom, slab), level) for k in steps]
    in_plane = []
    for k in range(1, group):
        other = lax.rem(place + k, group)
        in_plane.append((z * slab + other // levels, lax.rem(other, levels)))

    barrier = pltpu.get_barrier_semaphore()

    def greet(device):
        pl.semaphore_signal(barrier, inc=1, device_id=device, device_id_type=MESH)

    early = z < EARLY
    ahead = [lax.rem(z + k, PLANES) < EARLY for k in steps]
    for device in in_plane:
        greet(device)
    for other, device in zip(ahead, in_column):
        pl.when(early == other)(lambda device=device: greet(device))
    greeted = jnp.int32(len(in_plane)) + jnp.where(early, EARLY - 1, PLANES - 1)
    for there, device in zip(exists + [has_finer, has_coarser], near + [finer, coarser]):
        pl.when(there)(lambda device=device: greet(device))
        greeted = greeted + there.astype(jnp.int32)

    def remote(src, dst, send, recv, device):
        return pltpu.make_async_remote_copy(
            src_ref=src, dst_ref=dst, send_sem=send, recv_sem=recv, device_id=device, device_id_type=MESH
        )

    for o in range(slots):
        @pl.when(jnp.logical_not(exists[o]))
        def _():
            arrived[:, (o) * each : (o + 1) * each, :] = jnp.zeros((3, each, size), F32)

    @pl.when(jnp.logical_not(has_coarser))
    def _():
        child_in[...] = jnp.zeros(child_in.shape, F32)

    for copy in small[:3]:
        copy.wait()
    at_row = lax.broadcasted_iota(jnp.int32, mu.shape, 0) * 128
    at_row = at_row + lax.broadcasted_iota(jnp.int32, mu.shape, 1)
    alive = at_row < live[0, 0]
    mu_t = jnp.transpose(jnp.where(alive, mu[...], 0.0))
    lam_t = jnp.transpose(jnp.where(alive, lam[...], 0.0))
    for copy in stiffs:
        copy.wait()
    total = jnp.zeros((8, size), F32)
    n = CHUNK // 128
    for g in range(elements // CHUNK):
        if g * CHUNK in starts:
            loads[starts.index(g * CHUNK)].wait()
        rows = pl.ds(g * CHUNK, CHUNK)
        part = values[rows, :]
        a = jnp.concatenate([mu_t[:, g * n + i : g * n + i + 1] for i in range(n)], axis=0)
        b = jnp.concatenate([lam_t[:, g * n + i : g * n + i + 1] for i in range(n)], axis=0)
        for c in range(3):
            cols = slice(c * size, (c + 1) * size)
            pair = jnp.concatenate([stiff[0, :, cols], stiff[1, :, cols]], axis=1)
            both = jnp.dot(part, pair, preferred_element_type=F32)
            forces = a * both[:, :size] + b * both[:, size:]
            work = part[:, cols].astype(F32) * forces
            total = total + jnp.sum(work.reshape(CHUNK // 8, 8, size), axis=0)
            terms[c, rows, :] = split(forces)
    spark[...] = jnp.sum(total, axis=0, keepdims=True)
    for copy in small[3:]:
        copy.wait()

    column_copies = [
        remote(spark, column.at[k], column_send, column_recv, device) for k, device in enumerate(in_column)
    ]
    ask = remote(parents, wanted_in, wanted_sem.at[0], wanted_sem.at[1], coarser)
    shares = []
    for c in range(3):
        for o in range(slots):
            opposite = (o + half) % slots
            shares.append(
                remote(
                    gather.at[c, pl.ds(o * each, each), :], arrived.at[c, pl.ds(opposite * each, each), :],
                    share_send.at[c, o], share_recv.at[c, opposite], near[o],
                )
            )

    def meet():
        pl.semaphore_wait(barrier, greeted)
        for other, copy in zip(ahead, column_copies):
            pl.when(jnp.logical_not(early) | other)(copy.start)
        for other, device in zip(ahead, in_column):
            pl.when(early != other)(lambda device=device: greet(device))
        pl.when(has_coarser)(ask.start)

    def meet_far():
        pl.semaphore_wait(barrier, PLANES - EARLY)
        for other, copy in zip(ahead, column_copies):
            pl.when(jnp.logical_not(other))(copy.start)

    def send_shares(c):
        for o in range(slots):
            pl.when(exists[o])(shares[c * slots + o].start)

    plane_copies = [
        remote(plane_sum, plane.at[k], plane_send, plane_recv, device) for k, device in enumerate(in_plane)
    ]

    def pass_energy():
        remote(column, column, column_send, column_recv, finer).wait_recv()
        plane_sum[...] = spark[...] + jnp.sum(column[...], axis=0)
        for copy in plane_copies:
            copy.start()

    soon = early | (z >= FIRST)
    pl.when(soon)(meet)

    def sums(c):
        for i in range(count // TILE):
            hot = one_hot(i * TILE, TILE, ids[c : c + 1, :])
            both = jnp.dot(hot, terms[c], preferred_element_type=F32)
            out[c, i * TILE : (i + 1) * TILE, :] = both[:, :size] + both[:, size:]

    def pick(c):
        for o in range(slots):
            for s in range(each):
                row = jnp.minimum(share[o, s], count - 1)
                gather[c, o * each + s : o * each + s + 1, :] = out[c, pl.ds(row, 1), :]

    sums(0)
    pick(0)
    sums(1)
    pl.when(soon)(lambda: send_shares(0))
    pick(1)
    sums(2)
    pl.when(soon)(lambda: send_shares(1))
    pick(2)
    pl.when(soon)(lambda: send_shares(2))

    slot_ids = jnp.concatenate([slots_v[o : o + 1, :] for o in range(slots)], axis=1)
    hot[...] = one_hot(0, count, slot_ids)
    chosen = one_hot(0, count, children[...])
    hangs[...] = chosen
    keep[...] = jnp.broadcast_to(1.0 - jnp.sum(chosen.astype(F32), axis=1, keepdims=True), keep.shape)

    @pl.when(jnp.logical_not(soon))
    def _():
        meet()
        for c in range(3):
            send_shares(c)

    @pl.when(has_finer)
    def _():
        ask.wait_recv()
        fetch = pltpu.make_async_copy(wanted_in, wanted, wanted_sem.at[2])
        fetch.start()
        fetch.wait()

    sent = []
    for c in range(3):
        for o in range(slots):
            back = remote(
                gather.at[c, pl.ds(o * each, each), :], arrived.at[c, pl.ds(o * each, each), :],
                share_send.at[c, o], share_recv.at[c, o], near[o],
            )
            pl.when(exists[o])(back.wait_recv)
        both = jnp.dot(hot[...], split(arrived[c]), preferred_element_type=F32)
        out[c] = out[c] + (both[:, :size] + both[:, size:])
        copy = remote(child_out.at[c], child_in.at[c], child_send.at[c], child_recv.at[c], finer)
        sent.append(copy)

        @pl.when(has_finer)
        def _():
            def pair(h, carry):
                one = out[c, pl.ds(wanted[0, h], 1), :]
                two = out[c, pl.ds(wanted[1, h], 1), :]
                child_out[c, pl.ds(h, 1), :] = 0.5 * (one + two)
                return carry

            lax.fori_loop(0, wanted.shape[1], pair, 0, unroll=True)
            copy.start()

    pl.when(early)(meet_far)
    pass_energy()

    for c in range(3):
        pl.when(has_coarser)(sent[c].wait_recv)
        both = jnp.dot(hangs[...], split(child_in[c]), preferred_element_type=F32)
        out[c] = keep[...] * out[c] + (both[:, :size] + both[:, size:])

    for copy in column_copies:
        copy.wait_send()
    for c in range(3):
        for o in range(slots):
            pl.when(exists[o])(shares[c * slots + o].wait_send)
        pl.when(has_finer)(sent[c].wait_send)
    pl.when(has_coarser)(ask.wait_send)
    remote(plane, plane, plane_send, plane_recv, finer).wait_recv()
    everything = plane_sum[...] + jnp.sum(plane[...], axis=0)
    scale = 0.5 / (width * elements * ranks * levels)
    energy[...] = jnp.sum(everything, axis=1, keepdims=True) * scale
    for copy in plane_copies:
        copy.wait_send()


def shards(
    dg_values, stiff_mu, stiff_lam, coef_mu, coef_lam, elem_count, elem_block, share_map, hang_child, hang_parent
):
    elements, width = dg_values.shape
    size = width // 3
    count = elements // 3
    slots, each = share_map.shape[1:]
    hangs = hang_child.shape[1]
    group = lax.axis_size("dom") // PLANES * lax.axis_size("level")
    rows = elements // 128
    in_hbm = pl.BlockSpec(memory_space=pltpu.HBM)
    in_vmem = pl.BlockSpec(memory_space=VMEM)
    sem = pltpu.SemaphoreType.DMA
    i32 = jnp.int32
    projected, energy = pl.pallas_call(
        kernel,
        out_shape=[jax.ShapeDtypeStruct((3, count, size), F32), jax.ShapeDtypeStruct((1, 1), F32)],
        in_specs=[in_hbm] * 10,
        out_specs=[in_vmem, in_vmem],
        scratch_shapes=[
            pltpu.SMEM((1, 1), i32),
            VMEM((elements, width), BF16),
            VMEM((2, width, width), BF16),
            VMEM((rows, 128), F32),
            VMEM((rows, 128), F32),
            VMEM((3, elements), i32),
            pltpu.SMEM((slots, each), i32),
            VMEM((slots, each), i32),
            VMEM((2, hangs), i32),
            VMEM((1, hangs), i32),
            VMEM((3, elements, 2 * size), BF16),
            VMEM((3, slots * each, size), F32),
            VMEM((3, slots * each, size), F32),
            VMEM((3, hangs, size), F32),
            VMEM((3, hangs, size), F32),
            VMEM((2, hangs), i32),
            pltpu.SMEM((2, hangs), i32),
            VMEM((count, slots * each), BF16),
            VMEM((count, hangs), BF16),
            VMEM((count, size), F32),
            VMEM((1, size), F32),
            VMEM((PLANES - 1, 1, size), F32),
            VMEM((1, size), F32),
            VMEM((group - 1, 1, size), F32),
            sem((8,)), sem((2,)), sem((len(LOADS),)), sem((3, slots)), sem((3, slots)), sem((3,)), sem((3,)), sem((3,)),
            sem, sem, sem, sem,
        ],
        compiler_params=pltpu.CompilerParams(
            collective_id=0, has_side_effects=True, vmem_limit_bytes=24 * 2**20
        ),
    )(
        elem_count.reshape(1, 1),
        *(
            pltpu.with_memory_space_constraint(x, pltpu.HBM)
            for x in (
                dg_values, stiff_mu, stiff_lam, coef_mu.reshape(rows, 128), coef_lam.reshape(rows, 128),
                elem_block, share_map[0], jnp.transpose(hang_parent[0]), hang_child,
            )
        ),
    )
    return projected, energy[0, 0]


def solution(mesh):
    both = ("dom", "level")
    placed = (
        P(both, None), P(), P(), P(both), P(both), P(both), P(None, both),
        P(both, None, None), P(both, None), P(both, None, None),
    )
    return jax.shard_map(
        shards, mesh=mesh, in_specs=placed, out_specs=(P(None, both, None), P()), check_vma=False
    )
```
